64 devices in a mesh: data: 4 (over x, y), grp: 16 (over z, core).
Axes of the slice: x: 2, y: 2, z: 8, core: 2. Of those that a mesh axis runs over, the one named last changes fastest.
The devices are a block of a 4x4x8 slice.
Arguments:
- x_tokens: bfloat16 [4, 128, 1024], P('data', 'grp'), parts along dimension 0
- hint_tokens: bfloat16 [4, 128, 1024], P('data', 'grp'), parts along dimension 0
- target_noise: bfloat16 [4, 128, 1024], P('data', 'grp'), parts along dimension 0
- base_qkv: bfloat16 [2, 1024, 3072], replicated
- base_proj: bfloat16 [2, 1024, 1024], replicated
- base_up: bfloat16 [2, 1024, 4096], replicated
- base_down: bfloat16 [2, 4096, 1024], replicated
- ctrl_qkv: bfloat16 [2, 1024, 3072], replicated
- ctrl_proj: bfloat16 [2, 1024, 1024], replicated
- ctrl_up: bfloat16 [2, 1024, 4096], replicated
- ctrl_down: bfloat16 [2, 4096, 1024], replicated
- out_qkv: bfloat16 [1, 1024, 3072], replicated
- out_proj: bfloat16 [1, 1024, 1024], replicated
- out_up: bfloat16 [1, 1024, 4096], replicated
- out_down: bfloat16 [1, 4096, 1024], replicated
- skip_proj: bfloat16 [1, 2048, 1024], replicated
- hint_proj: bfloat16 [1024, 1024], replicated
- zero_proj: bfloat16 [2, 1024, 1024], replicated
- head_proj: bfloat16 [1024, 1024], replicated
Outputs:
- output 1: float32 [4], P('data'), parts along dimension 0
- output 2: bfloat16 [8, 1024, 3072], P('data', 'grp'), parts along dimension 0
- output 3: bfloat16 [8, 1024, 1024], P('data', 'grp'), parts along dimension 0
- output 4: bfloat16 [8, 1024, 4096], P('data', 'grp'), parts along dimension 0
- output 5: bfloat16 [8, 4096, 1024], P('data', 'grp'), parts along dimension 0
- output 6: bfloat16 [4096, 1024], P(('data', 'grp')), parts along dimension 0
- output 7: bfloat16 [8, 1024, 1024], P('data', 'grp'), parts along dimension 0
There are 4 independent parts. The reference program is written for one: setup_inputs(seed, part) draws one part's arguments, and reference() takes and returns one part's arrays. A program takes and returns all parts, laid end to end along the dimension named above; an argument that names none is the same for every part.
All inputs are finite; a program needn't handle non-finite values.
Results may differ from the reference program's by a relative error of at most 0.02.
Values are sent between devices in bfloat16 or wider.
A program may use at most 768 MiB of HBM per device.

```python
import jax
import jax.numpy as jnp
from jax import lax

PART_BATCH = 1
SEQ_LEN = 128
MODEL_DIM = 1024
IN_BLOCKS = 1
HEAD_DIM = 64

NUM_HEADS = MODEL_DIM // HEAD_DIM
NORM_EPS = 1e-6
ZERO_GAIN = 0.6


def draw_normal(rng_key, dim_list, fan_in, gain_val):
    vals_f32 = jax.random.normal(rng_key, dim_list, jnp.float32) * (gain_val * fan_in ** -0.5)
    return vals_f32.astype(jnp.bfloat16)


def block_set(weight_keys, first_key, num_blocks):
    model_dim = MODEL_DIM
    return [
        draw_normal(weight_keys[first_key], (num_blocks, model_dim, 3 * model_dim), model_dim, 1.0),
        draw_normal(weight_keys[first_key + 1], (num_blocks, model_dim, model_dim), model_dim, 1.0),
        draw_normal(weight_keys[first_key + 2], (num_blocks, model_dim, 4 * model_dim), model_dim, 1.0),
        draw_normal(weight_keys[first_key + 3], (num_blocks, 4 * model_dim, model_dim), 4 * model_dim, 1.0),
    ]


def setup_inputs(seed: int = 0, part: int = 0) -> dict:
    part_key = jax.random.fold_in(jax.random.key(seed), part)
    act_keys = jax.random.split(part_key, 3)
    weight_keys = jax.random.split(jax.random.key(seed + 1), 16)
    act_shape = (PART_BATCH, SEQ_LEN, MODEL_DIM)
    stacks = IN_BLOCKS + 1
    base_set = block_set(weight_keys, 0, stacks)
    ctrl_set = block_set(weight_keys, 4, stacks)
    out_set = block_set(weight_keys, 8, IN_BLOCKS)
    return {
        'x_tokens': jax.random.normal(act_keys[0], act_shape, jnp.float32).astype(jnp.bfloat16),
        'hint_tokens': jax.random.normal(act_keys[1], act_shape, jnp.float32).astype(jnp.bfloat16),
        'target_noise': jax.random.normal(act_keys[2], act_shape, jnp.float32).astype(jnp.bfloat16),
        'base_qkv': base_set[0],
        'base_proj': base_set[1],
        'base_up': base_set[2],
        'base_down': base_set[3],
        'ctrl_qkv': ctrl_set[0],
        'ctrl_proj': ctrl_set[1],
        'ctrl_up': ctrl_set[2],
        'ctrl_down': ctrl_set[3],
        'out_qkv': out_set[0],
        'out_proj': out_set[1],
        'out_up': out_set[2],
        'out_down': out_set[3],
        'skip_proj': draw_normal(weight_keys[12], (IN_BLOCKS, 2 * MODEL_DIM, MODEL_DIM), 2 * MODEL_DIM, 1.0),
        'hint_proj': draw_normal(weight_keys[13], (MODEL_DIM, MODEL_DIM), MODEL_DIM, 1.0),
        'zero_proj': draw_normal(weight_keys[14], (stacks, MODEL_DIM, MODEL_DIM), MODEL_DIM, ZERO_GAIN),
        'head_proj': draw_normal(weight_keys[15], (MODEL_DIM, MODEL_DIM), MODEL_DIM, 1.0),
    }


def norm_f32(vals_f32):
    mean_val = jnp.mean(vals_f32, axis=-1, keepdims=True)
    centered = vals_f32 - mean_val
    variance = jnp.mean(centered * centered, axis=-1, keepdims=True)
    return centered * lax.rsqrt(variance + NORM_EPS)


def layer_norm(resid_act):
    return norm_f32(resid_act.astype(jnp.float32)).astype(jnp.bfloat16)


def matmul(left, right):
    return jnp.dot(left, right, preferred_element_type=jnp.float32)


def block(resid_act, w_qkv, w_proj, w_up, w_down):
    num_batch, num_tok, model_dim = resid_act.shape
    qkv_out = matmul(layer_norm(resid_act), w_qkv).astype(jnp.bfloat16)
    heads_view = qkv_out.astype(jnp.float32).reshape(num_batch, num_tok, 3, NUM_HEADS, HEAD_DIM)
    scores = jnp.einsum('bqhe,bkhe->bhqk', heads_view[:, :, 0], heads_view[:, :, 1]) * HEAD_DIM ** -0.5
    attn_probs = jax.nn.softmax(scores, axis=-1).astype(jnp.bfloat16).astype(jnp.float32)
    context = jnp.einsum('bhqk,bkhe->bqhe', attn_probs, heads_view[:, :, 2]).astype(jnp.bfloat16)
    u_one = (resid_act.astype(jnp.float32) + matmul(context.reshape(num_batch, num_tok, model_dim), w_proj)).astype(jnp.bfloat16)
    hidden = jax.nn.gelu(matmul(layer_norm(u_one), w_up), approximate=True).astype(jnp.bfloat16)
    return (u_one.astype(jnp.float32) + matmul(hidden, w_down)).astype(jnp.bfloat16)


def forward_loss(ctrl_params, x_tokens, hint_tokens, target_noise, base_set, out_set, skip_proj, head_proj):
    ctrl_qkv, ctrl_proj, ctrl_up, ctrl_down, hint_proj, zero_proj = ctrl_params
    ckpt_block = jax.checkpoint(block)

    def base_step(resid_act, weights):
        new_resid = ckpt_block(resid_act, weights[0], weights[1], weights[2], weights[3])
        return new_resid, new_resid

    base_in = tuple(stack_arr[:IN_BLOCKS] for stack_arr in base_set)
    base_last, skip_acts = lax.scan(base_step, x_tokens, base_in)
    mid_out = ckpt_block(base_last, base_set[0][IN_BLOCKS], base_set[1][IN_BLOCKS], base_set[2][IN_BLOCKS], base_set[3][IN_BLOCKS])
    ctrl_start = (x_tokens.astype(jnp.float32) + matmul(hint_tokens, hint_proj)).astype(jnp.bfloat16)

    def ctrl_step(resid_act, weights):
        new_resid = ckpt_block(resid_act, weights[0], weights[1], weights[2], weights[3])
        return new_resid, matmul(new_resid, weights[4]).astype(jnp.bfloat16)

    ctrl_in = (ctrl_qkv[:IN_BLOCKS], ctrl_proj[:IN_BLOCKS], ctrl_up[:IN_BLOCKS], ctrl_down[:IN_BLOCKS], zero_proj[:IN_BLOCKS])
    ctrl_last, residuals = lax.scan(ctrl_step, ctrl_start, ctrl_in)
    ctrl_mid = ckpt_block(ctrl_last, ctrl_qkv[IN_BLOCKS], ctrl_proj[IN_BLOCKS], ctrl_up[IN_BLOCKS], ctrl_down[IN_BLOCKS])
    mid_res = matmul(ctrl_mid, zero_proj[IN_BLOCKS]).astype(jnp.bfloat16)
    out_resid = (mid_out.astype(jnp.float32) + mid_res.astype(jnp.float32)).astype(jnp.bfloat16)
    skip_sums = (skip_acts.astype(jnp.float32) + residuals.astype(jnp.float32)).astype(jnp.bfloat16)[::-1]

    def out_step(resid_act, weights):
        joined = jnp.concatenate([resid_act, weights[5]], axis=-1)
        merged = matmul(joined, weights[4]).astype(jnp.bfloat16)
        return ckpt_block(merged, weights[0], weights[1], weights[2], weights[3]), None

    out_resid = lax.scan(out_step, out_resid, (out_set[0], out_set[1], out_set[2], out_set[3], skip_proj, skip_sums))[0]
    pred_out = matmul(layer_norm(out_resid), head_proj).astype(jnp.bfloat16)
    pred_err = pred_out.astype(jnp.float32) - target_noise.astype(jnp.float32)
    per_sample = jnp.mean(pred_err * pred_err, axis=(1, 2))
    return jnp.mean(per_sample), per_sample


def reference(x_tokens, hint_tokens, target_noise, base_qkv, base_proj, base_up, base_down, ctrl_qkv, ctrl_proj, ctrl_up, ctrl_down, out_qkv, out_proj, out_up, out_down, skip_proj, hint_proj, zero_proj, head_proj):
    ctrl_params = (ctrl_qkv, ctrl_proj, ctrl_up, ctrl_down, hint_proj, zero_proj)
    base_set = (base_qkv, base_proj, base_up, base_down)
    out_set = (out_qkv, out_proj, out_up, out_down)

    def loss_fn(params):
        return forward_loss(params, x_tokens, hint_tokens, target_noise, base_set, out_set, skip_proj, head_proj)

    loss_pair, grad_list = jax.value_and_grad(loss_fn, has_aux=True)(ctrl_params)
    return (loss_pair[1], grad_list[0], grad_list[1], grad_list[2], grad_list[3], grad_list[4], grad_list[5])
```

```python
import jax
import jax.numpy as jnp
from jax import lax
from jax.sharding import PartitionSpec as P

HEAD_DIM = 64
NORM_EPS = 1e-6


def mm(left, right):
    return jnp.einsum('td,de->te', left, right, preferred_element_type=jnp.float32)


def mm_back(grad_bf, right):
    return jnp.einsum('te,de->td', grad_bf, right, preferred_element_type=jnp.float32)


def norm_f32(vals_f32):
    mean_val = jnp.mean(vals_f32, axis=-1, keepdims=True)
    centered = vals_f32 - mean_val
    variance = jnp.mean(centered * centered, axis=-1, keepdims=True)
    return centered * lax.rsqrt(variance + NORM_EPS)


def layer_norm(resid_act):
    return norm_f32(resid_act.astype(jnp.float32)).astype(jnp.bfloat16)


def norm_vjp(resid_act, grad_norm):
    return jax.vjp(norm_f32, resid_act.astype(jnp.float32))[1](grad_norm)[0]


def gelu_tanh(pre_vals):
    return jax.nn.gelu(pre_vals, approximate=True)


def softmax_probs(query_h, keys_all):
    scores = jnp.einsum('qhe,khe->hqk', query_h, keys_all, preferred_element_type=jnp.float32) * HEAD_DIM ** -0.5
    return jax.nn.softmax(scores, axis=-1)


def block_fwd(resid_in, weights):
    w_qkv, w_proj, w_up, w_down = weights
    num_tok, model_dim = resid_in.shape
    num_heads = model_dim // HEAD_DIM
    qkv_out = mm(layer_norm(resid_in), w_qkv).astype(jnp.bfloat16)
    split = lambda k: qkv_out[:, k * model_dim:(k + 1) * model_dim].reshape(num_tok, num_heads, HEAD_DIM)
    query_h, keys_all, vals_all = split(0), split(1), split(2)
    attn_probs = softmax_probs(query_h, keys_all).astype(jnp.bfloat16)
    context = jnp.einsum('hqk,khe->qhe', attn_probs, vals_all, preferred_element_type=jnp.float32).astype(jnp.bfloat16).reshape(num_tok, model_dim)
    u_one = (resid_in.astype(jnp.float32) + mm(context, w_proj)).astype(jnp.bfloat16)
    pre_act = mm(layer_norm(u_one), w_up)
    hidden = gelu_tanh(pre_act).astype(jnp.bfloat16)
    u_two = (u_one.astype(jnp.float32) + mm(hidden, w_down)).astype(jnp.bfloat16)
    return u_two, (resid_in, query_h, keys_all, vals_all, context, u_one, pre_act)


def block_bwd(grad_out, saved_acts, weights, own_rows, need_weights):
    resid_in, query_h, keys_all, vals_all, context, u_one, pre_act = saved_acts
    w_qkv, w_proj, w_up, w_down = weights
    num_tok, model_dim = resid_in.shape
    grad_bf = grad_out.astype(jnp.bfloat16)
    g_hidden = mm_back(grad_bf, w_down)
    g_pre = jax.vjp(gelu_tanh, pre_act)[1](g_hidden)[0].astype(jnp.bfloat16)
    g_one = grad_out + norm_vjp(u_one, mm_back(g_pre, w_up))
    g_one_bf = g_one.astype(jnp.bfloat16)
    g_context = mm_back(g_one_bf, w_proj).astype(jnp.bfloat16).reshape(num_tok, model_dim // HEAD_DIM, HEAD_DIM)
    attn_probs = softmax_probs(query_h, keys_all)
    probs_bf = attn_probs.astype(jnp.bfloat16)
    g_probs = jnp.einsum('qhe,khe->hqk', g_context, vals_all, preferred_element_type=jnp.float32)
    g_vals = jnp.einsum('hqk,qhe->khe', probs_bf, g_context, preferred_element_type=jnp.float32)
    g_scores = (attn_probs * (g_probs - jnp.sum(g_probs * attn_probs, axis=-1, keepdims=True)) * HEAD_DIM ** -0.5).astype(jnp.bfloat16)
    g_query = jnp.einsum('hqk,khe->qhe', g_scores, keys_all, preferred_element_type=jnp.float32)
    g_keys = jnp.einsum('hqk,qhe->khe', g_scores, query_h, preferred_element_type=jnp.float32)
    flat = lambda v: v.reshape(num_tok, model_dim).astype(jnp.bfloat16)
    g_qkv_out = jnp.concatenate([flat(g_query), flat(g_keys), flat(g_vals)], axis=-1)
    g_in = g_one + norm_vjp(resid_in, mm_back(g_qkv_out, w_qkv))
    if need_weights:
        hidden = gelu_tanh(pre_act).astype(jnp.bfloat16)
        return g_in, (
            own_rows(layer_norm(resid_in), g_qkv_out),
            own_rows(context, g_one_bf),
            own_rows(layer_norm(u_one), g_pre),
            own_rows(hidden, grad_bf),
        )
    return g_in, None


def solution(mesh):
    group_size = mesh.shape['grp']
    act_spec = P('data', 'grp', None)
    stack_spec = P('data', 'grp', None)

    def local_step(x_tokens, hint_tokens, target_noise, base_qkv, base_proj, base_up, base_down, ctrl_qkv, ctrl_proj, ctrl_up, ctrl_down, out_qkv, out_proj, out_up, out_down, skip_proj, hint_proj, zero_proj, head_proj):
        pos = lax.axis_index('grp')
        num_in = skip_proj.shape[0]
        model_dim = x_tokens.shape[2]
        stacked_in = jnp.concatenate([x_tokens, hint_tokens, target_noise], axis=0)
        gathered = lax.all_gather(stacked_in, 'grp', axis=1, tiled=True)
        x_all, hint_all, target_all = gathered[0], gathered[1], gathered[2]
        seq_len = x_all.shape[0]

        def own_rows(left, grad_bf):
            width = left.shape[1] // group_size
            mine = lax.dynamic_slice_in_dim(left, pos * width, width, axis=1)
            return jnp.einsum('td,te->de', mine, grad_bf, preferred_element_type=jnp.float32).astype(jnp.bfloat16)

        base_set = (base_qkv, base_proj, base_up, base_down)
        ctrl_set = (ctrl_qkv, ctrl_proj, ctrl_up, ctrl_down)
        out_set = (out_qkv, out_proj, out_up, out_down)
        pick = lambda group, idx: tuple(stack[idx] for stack in group)
        f32 = jnp.float32
        bf16 = jnp.bfloat16

        base_outs, ctrl_outs, ctrl_saved, residuals = [], [], [], []
        base_act = x_all
        ctrl_act = (x_all.astype(f32) + mm(hint_all, hint_proj)).astype(bf16)
        for idx in range(num_in + 1):
            base_act = block_fwd(base_act, pick(base_set, idx))[0]
            ctrl_act, saved = block_fwd(ctrl_act, pick(ctrl_set, idx))
            base_outs.append(base_act)
            ctrl_outs.append(ctrl_act)
            ctrl_saved.append(saved)
            residuals.append(mm(ctrl_act, zero_proj[idx]).astype(bf16))
        out_act = (base_outs[num_in].astype(f32) + residuals[num_in].astype(f32)).astype(bf16)
        out_saved = []
        for idx in range(num_in):
            src = num_in - 1 - idx
            skip_sum = (base_outs[src].astype(f32) + residuals[src].astype(f32)).astype(bf16)
            merged = mm(jnp.concatenate([out_act, skip_sum], axis=-1), skip_proj[idx]).astype(bf16)
            out_act, saved = block_fwd(merged, pick(out_set, idx))
            out_saved.append(saved)
        pred_out = mm(layer_norm(out_act), head_proj).astype(bf16)
        pred_err = pred_out.astype(f32) - target_all.astype(f32)
        per_sample = (jnp.sum(pred_err * pred_err) / (seq_len * model_dim)).reshape(1)
        g_pred = (pred_err * (2.0 / (seq_len * model_dim))).astype(bf16)
        g_out = norm_vjp(out_act, mm_back(g_pred, head_proj))
        g_res = [None] * (num_in + 1)
        for idx in reversed(range(num_in)):
            g_merged = block_bwd(g_out, out_saved[idx], pick(out_set, idx), own_rows, False)[0]
            g_joined = mm_back(g_merged.astype(bf16), skip_proj[idx])
            g_out = g_joined[:, :model_dim]
            g_res[num_in - 1 - idx] = g_joined[:, model_dim:].astype(bf16)
        g_res[num_in] = g_out.astype(bf16)
        g_act = jnp.zeros(x_all.shape, f32)
        zero_grads = [None] * (num_in + 1)
        block_grads = [None] * (num_in + 1)
        for idx in reversed(range(num_in + 1)):
            g_act = g_act + mm_back(g_res[idx], zero_proj[idx])
            zero_grads[idx] = own_rows(ctrl_outs[idx], g_res[idx])
            g_act, block_grads[idx] = block_bwd(g_act, ctrl_saved[idx], pick(ctrl_set, idx), own_rows, True)
        g_hint = own_rows(hint_all, g_act.astype(bf16))
        stacked = [jnp.stack([grads[k] for grads in block_grads]) for k in range(4)]
        return (per_sample, stacked[0], stacked[1], stacked[2], stacked[3], g_hint, jnp.stack(zero_grads))

    in_specs = (act_spec, act_spec, act_spec) + tuple(P() for spec_idx in range(16))
    out_specs = (P('data'), stack_spec, stack_spec, stack_spec, stack_spec, P(('data', 'grp'), None), stack_spec)
    return jax.shard_map(local_step, mesh=mesh, in_specs=in_specs, out_specs=out_specs, check_vma=False)
```
